32 devices in a mesh: tm: 16 (over z, x, core), tile: 2 (over y).
Axes of the slice: x: 2, y: 2, z: 4, core: 2. Of those that a mesh axis runs over, the one named last changes fastest.
Arguments:
- queries: bfloat16 [32, 4, 64, 2560], P('tm', 'tile'), may hold values from -40 to 40
- keys: bfloat16 [32, 4, 64, 2560], P('tm', 'tile'), may hold values from -6 to 6
- values: bfloat16 [32, 4, 64, 2560], P('tm', 'tile'), may hold values from -6 to 6
- neighbours: int32 [16, 2, 3], P('tm', 'tile'), may hold values from -1 to 14, as said below
- halo_rows: int32 [16, 2], P('tm', 'tile'), may hold values from 0 to 2, as said below
Outputs:
- attended: bfloat16 [32, 4, 64, 2560], P('tm', 'tile')
The draws below stay inside these ranges and needn't reach their ends.
Inputs may be any that keep to these rules, and one draw needn't show every extreme that they name: `neighbours`: for frame block b and tile t, the entries that are not -1 are distinct frame blocks from max(0, b - 5) to b - 1; lists hold 0 to 3 entries, and some list is full. `halo_rows`: some frame block and tile reads 2 rows.
All inputs are finite; a program needn't handle non-finite values.
Results may differ from the reference program's by a relative error of at most 0.0046.
Values may be sent and summed in bfloat16 or wider, within the bound.
A program may use at most 128 MiB of HBM per device.

```python
import math
import jax
import jax.numpy as jnp
from jax import lax

HEADS = 20
HD = 128
GRID_W = 64
FR_DEV = 2
TROWS = 2
HMAX = 2
NB = 3
WIN = 5
CHANNELS = 2560
BLOCKS = 16
TILES = 2
FRAMES = 32
GRID_H = 4


def drawn_pair(key):
    base = jax.random.fold_in(key, 11)
    query_seed, keys_seed = jax.random.split(base, 2)
    shape = (FRAMES, GRID_H, GRID_W, HEADS, HD)
    query_base = jnp.clip(jax.random.normal(query_seed, shape, jnp.float32), -6.0, 6.0)
    key_base = jnp.clip(jax.random.normal(keys_seed, shape, jnp.float32), -6.0, 6.0)
    flat_shape = (FRAMES, GRID_H, GRID_W, HEADS * HD)
    return (query_base.reshape(flat_shape), key_base.reshape(flat_shape))


def draw_queries(key, part):
    return drawn_pair(key)[0].astype(jnp.bfloat16)


def draw_keys(key, part):
    return drawn_pair(key)[1].astype(jnp.bfloat16)


def draw_neighbours(key, part):
    base = jax.random.fold_in(key, 31)
    bits_seed, length_seed = jax.random.split(base)
    random_bits = jax.random.randint(bits_seed, (BLOCKS, TILES, WIN), 0, 1 << 20)
    offsets = jnp.arange(1, WIN + 1, dtype=jnp.int32)
    block_pos = jnp.arange(BLOCKS, dtype=jnp.int32)[:, None, None]
    usable = block_pos - offsets[None, None, :] >= 0
    ranked = jnp.where(usable, random_bits * WIN + offsets - 1 + WIN, offsets - 1 + jnp.zeros_like(random_bits))
    top_vals, top_idx = lax.top_k(ranked, NB)
    chosen = top_idx.astype(jnp.int32) + 1
    list_length = jax.random.randint(length_seed, (BLOCKS, TILES), 0, NB + 1)
    list_length = list_length.at[BLOCKS - 1, 0].set(NB)
    slot_index = jnp.arange(NB, dtype=jnp.int32)[None, None, :]
    block_ids = block_pos - chosen
    kept_mask = (slot_index < list_length[:, :, None]) & (block_ids >= 0)
    return jnp.where(kept_mask, block_ids, -1).astype(jnp.int32)


def draw_halo_rows(key, part):
    widths = jax.random.randint(jax.random.fold_in(key, 23), (BLOCKS, TILES), 0, HMAX + 1)
    return widths.at[BLOCKS - 1, 0].set(HMAX).astype(jnp.int32)


def levels(key, shape, pieces, low, high):
    level, own = 1.0, jax.random.fold_in(key, 6)
    for axis_at, shards_of in pieces:
        draws = jnp.exp(jax.random.uniform(jax.random.fold_in(own, axis_at), (shards_of,), jnp.float32, low / len(pieces), high / len(pieces)))
        level = level * jnp.repeat(draws, shape[axis_at] // shards_of).reshape([-1 if axis == axis_at else 1 for axis in range(len(shape))])
    return level


def normal_values(key, shape, spread, bound, cuts=(), kind=jnp.bfloat16):
    factor_of = levels(key, shape, cuts, -0.22, 0.18) if cuts else 1.0
    array = jax.random.normal(key, shape, jnp.float32) * spread * factor_of
    return jnp.minimum(jnp.maximum(array, -bound), bound).astype(kind)


def setup_inputs(seed: int = 0) -> dict:
    key_list = jax.random.split(jax.random.key(seed), 6)
    return {
        "queries": draw_queries(jax.random.fold_in(key_list[5], 71), 0),
        "keys": draw_keys(jax.random.fold_in(key_list[5], 71), 0),
        "values": normal_values(key_list[2], (FRAMES, GRID_H, GRID_W, CHANNELS), 1.0, 6.0, ((0, 16), (1, 2))),
        "neighbours": draw_neighbours(jax.random.fold_in(key_list[5], 71), 0),
        "halo_rows": draw_halo_rows(jax.random.fold_in(key_list[5], 71), 0),
    }


def attend(query_rows, key_rows, value_rows, allowed):
    tokens, channels = query_rows.shape
    head_count = channels // HD
    key_count = key_rows.shape[0]
    query_heads = query_rows.astype(jnp.float32).reshape(tokens, head_count, HD)
    key_heads = key_rows.astype(jnp.float32).reshape(key_count, head_count, HD)
    value_heads = value_rows.astype(jnp.float32).reshape(key_count, head_count, HD)
    scores = jnp.einsum('qhd,khd->hqk', query_heads, key_heads) / math.sqrt(HD)
    scores = jnp.where(allowed[None], scores, -jnp.inf)
    maximum = lax.optimization_barrier(jnp.max(scores, axis=2, keepdims=True))
    weights = jnp.where(allowed[None], jnp.exp(scores - maximum), 0.0)
    totals = lax.optimization_barrier(jnp.sum(weights, axis=2))
    rounded = lax.optimization_barrier(weights.astype(jnp.bfloat16)).astype(jnp.float32)
    numerator = jnp.einsum('hqk,khd->qhd', rounded, value_heads)
    return (numerator / totals.T[:, :, None]).reshape(tokens, channels).astype(jnp.bfloat16)

def reference(queries, keys, values, neighbours, halo_rows):
    channels = queries.shape[3]
    tokens = FR_DEV * TROWS * GRID_W
    span_rows = TROWS + 2 * HMAX
    pad_keys = jnp.pad(keys, ((0, 0), (HMAX, HMAX), (0, 0), (0, 0)))
    pad_values = jnp.pad(values, ((0, 0), (HMAX, HMAX), (0, 0), (0, 0)))
    anchor = jnp.zeros((), jnp.int32)
    query_frame = lax.broadcasted_iota(jnp.int32, (FR_DEV, TROWS, GRID_W), 0).reshape(-1)
    key_frame = lax.broadcasted_iota(jnp.int32, (FR_DEV, span_rows, GRID_W), 0).reshape(-1)
    key_row = lax.broadcasted_iota(jnp.int32, (FR_DEV, span_rows, GRID_W), 1).reshape(-1)

    def one_device(device):
        block_index = (device // TILES).astype(jnp.int32)
        tile_index = (device % TILES).astype(jnp.int32)
        frame_start = (block_index * FR_DEV).astype(jnp.int32)
        row_start = (tile_index * TROWS).astype(jnp.int32)
        query_rows = lax.dynamic_slice(queries, (frame_start, row_start, anchor, anchor), (FR_DEV, TROWS, GRID_W, channels)).reshape(tokens, channels)
        own_keys = lax.dynamic_slice(pad_keys, (frame_start, row_start, anchor, anchor), (FR_DEV, span_rows, GRID_W, channels)).reshape(-1, channels)
        own_values = lax.dynamic_slice(pad_values, (frame_start, row_start, anchor, anchor), (FR_DEV, span_rows, GRID_W, channels)).reshape(-1, channels)
        listed = neighbours[block_index, tile_index]
        halo_reach = halo_rows[block_index, tile_index]

        def fetch_rows(block_id):
            start_frame = (jnp.maximum(block_id, 0) * FR_DEV).astype(jnp.int32)
            far_keys = lax.dynamic_slice(keys, (start_frame, row_start, anchor, anchor), (FR_DEV, TROWS, GRID_W, channels))
            far_values = lax.dynamic_slice(values, (start_frame, row_start, anchor, anchor), (FR_DEV, TROWS, GRID_W, channels))
            return (far_keys, far_values)
        far_keys, far_values = jax.vmap(fetch_rows)(listed)
        global_row = row_start - HMAX + key_row
        row_ok = (global_row >= 0) & (global_row < GRID_H) & (key_row >= HMAX - halo_reach) & (key_row < HMAX + TROWS + halo_reach)
        own_mask = (key_frame[None, :] <= query_frame[:, None]) & row_ok[None, :]
        slot_mask = jnp.repeat(listed >= 0, tokens)
        allowed = jnp.concatenate((own_mask, jnp.broadcast_to(slot_mask[None, :], (tokens, slot_mask.shape[0]))), axis=1)
        key_rows = jnp.concatenate((own_keys, far_keys.reshape(-1, channels)), axis=0)
        value_rows = jnp.concatenate((own_values, far_values.reshape(-1, channels)), axis=0)
        return attend(query_rows, key_rows, value_rows, allowed)
    results = lax.map(one_device, jnp.arange(BLOCKS * TILES, dtype=jnp.int32))
    results = results.reshape(BLOCKS, TILES, FR_DEV, TROWS, GRID_W, channels)
    return results.transpose(0, 2, 1, 3, 4, 5).reshape(FRAMES, GRID_H, GRID_W, channels)
```

```python
import functools
import math

import jax
import jax.numpy as jnp
from jax import lax
from jax.experimental import pallas as pl
from jax.experimental.pallas import tpu as pltpu
from jax.sharding import PartitionSpec as P

HD = 128
HMAX = 2
WIN = 5
UP, DOWN = WIN + 1, WIN + 2
SLOTS = WIN + 3
AHEAD = 2
LOW = -1e30
SCALE = math.log2(math.e) / math.sqrt(HD)

ROUTES = (
    ((0, 0, 4, None), (0, 0, 2, None), (0, 0, 1, None), (1, 4, 5, None), (1, 2, 3, None)),
    (
        (0, 0, 2, None),
        (0, 0, 4, 0),
        (1, 2, 5, 1),
        (1, 4, 5, 0),
        (1, 2, 1, None),
        (1, 4, 3, 0),
        (2, 5, 3, 1),
        (3, 3, 4, 1),
    ),
    ((0, 0, 4, None), (0, 0, 1, None), (1, 4, 2, None), (1, 4, 5, None), (2, 2, 3, None)),
    ((0, 0, 4, None), (1, 4, 2, None), (1, 4, 3, None), (2, 2, 5, None), (2, 2, 1, None)),
)
GROUP = len(ROUTES)
STAGES = 4


def sends_of(role):
    found = []
    for origin, rows in enumerate(ROUTES):
        for stage, src, dst, parity in rows:
            if (origin + src) % GROUP == role:
                found.append((stage, src, dst - src, dst, parity))
    return found


MOST = max(len(sends_of(role)) for role in range(GROUP))


def both(*terms):
    out = terms[0]
    for term in terms[1:]:
        out = jnp.logical_and(out, term)
    return out


def kernel(count, tiles, shape, lists_ref, halo_ref, q_ref, k_ref, v_ref, out_ref,
           kv, q_v, bias, local_sem, q_sem, send_sem, recv_sem):
    frames, rows, columns = shape
    tokens = frames * rows * columns
    heads = q_ref.shape[1] // HD
    block = lax.axis_index("tm")
    tile = lax.axis_index("tile")
    role = block % GROUP

    def part(ref, head):
        return ref.at[:, pl.ds(pl.multiple_of(head * HD, HD), HD)]

    def fetch(head, carry):
        pltpu.make_async_copy(part(k_ref, head), kv.at[0, head, 0], local_sem.at[head]).start()
        pltpu.make_async_copy(part(v_ref, head), kv.at[0, head, 1], local_sem.at[head]).start()
        return carry

    lax.fori_loop(0, heads, fetch, 0)
    q_copy = pltpu.make_async_copy(q_ref, q_v, q_sem)
    q_copy.start()

    barrier = pltpu.get_barrier_semaphore()
    expected = jnp.int32(0)
    partners = [("tm", block, count, step) for step in range(-WIN, WIN + 1) if step]
    partners += [("tile", tile, tiles, step) for step in (-1, 1)]
    for axis, me, size, step in partners:
        there = both(me + step >= 0, me + step < size)

        @pl.when(there)
        def _():
            pl.semaphore_signal(barrier, inc=1, device_id={axis: me + step},
                                device_id_type=pl.DeviceIdType.MESH)

        expected += there.astype(jnp.int32)

    missing = [(d, block < d) for d in range(1, WIN + 1)]
    missing += [(UP, tile < 1), (DOWN, tile + 1 >= tiles)]
    for slot, gone in missing:

        @pl.when(gone)
        def _():
            def clear(head, carry):
                kv[slot, head] = jnp.zeros(kv.shape[2:], kv.dtype)
                return carry

            lax.fori_loop(0, heads, clear, 0)

    reach = halo_ref[0]
    query = lax.broadcasted_iota(jnp.int32, (tokens, tokens), 0) // (rows * columns)
    key = lax.broadcasted_iota(jnp.int32, (tokens, tokens), 1)
    key_row = (key // columns) % rows
    causal = key // (rows * columns) <= query
    above = both(causal, key_row >= rows - reach, tile >= 1)
    below = both(causal, key_row < reach, tile + 1 < tiles)
    for at, mask in enumerate((causal, above, below)):
        bias[at] = jnp.where(mask, 0.0, LOW)

    present = []
    for d in range(1, WIN + 1):
        hit = lists_ref[0] == block - d
        for n in range(1, lists_ref.shape[0]):
            hit = jnp.logical_or(hit, lists_ref[n] == block - d)
        present.append(jnp.logical_and(hit, block >= d))

    pl.semaphore_wait(barrier, expected)

    def remote(src, dst, head, sem, target):
        return pltpu.make_async_remote_copy(
            src_ref=kv.at[src, head],
            dst_ref=kv.at[dst, head],
            send_sem=send_sem.at[sem],
            recv_sem=recv_sem.at[dst, head],
            device_id=target,
            device_id_type=pl.DeviceIdType.MESH,
        )

    def arrived(slot, head):
        remote(slot, slot, head, 0, {"tm": block}).wait_recv()

    def own(head):
        pltpu.make_async_copy(kv.at[0, head], kv.at[0, head], local_sem.at[head]).wait()

        @pl.when(tile + 1 < tiles)
        def _():
            remote(0, UP, head, MOST, {"tile": tile + 1}).start()

        @pl.when(tile >= 1)
        def _():
            remote(0, DOWN, head, MOST + 1, {"tile": tile - 1}).start()

        relay(0, head)

    def relay(stage, head):
        for mine in range(GROUP):
            entries = [(at, *e) for at, e in enumerate(sends_of(mine)) if e[0] == stage]
            if not entries:
                continue

            @pl.when(role == mine)
            def _():
                for slot in sorted({e[2] for e in entries}):
                    group = [e for e in entries if e[2] == slot]
                    parities = {e[5] for e in group}
                    if slot:
                        needed = block >= slot
                        if None not in parities:
                            needed = both(needed, head % 2 == min(parities))

                        @pl.when(needed)
                        def _():
                            arrived(slot, head)

                    for at, _, _, step, dst, parity in group:
                        go = both(block >= slot, block + step < count)
                        if parity is not None:
                            go = both(go, head % 2 == parity)

                        @pl.when(go)
                        def _():
                            remote(slot, dst, head, at, {"tm": block + step}).start()

    def leaves(head):
        for mine in range(GROUP):
            entries = sends_of(mine)

            @pl.when(role == mine)
            def _():
                for slot in range(1, WIN + 1):
                    parities = {e[4] for e in entries if e[1] == slot}
                    if None in parities or parities == {0, 1}:
                        continue
                    needed = block >= slot
                    if parities:
                        needed = both(needed, head % 2 != min(parities))

                    @pl.when(needed)
                    def _():
                        arrived(slot, head)

        @pl.when(tile >= 1)
        def _():
            arrived(UP, head)

        @pl.when(tile + 1 < tiles)
        def _():
            arrived(DOWN, head)

    def attend(head):
        query_part = part(q_v, head)[...]
        scores = []
        tops = []
        for slot in range(SLOTS):
            s = lax.dot_general(query_part, kv[slot, head, 0], (((1,), (1,)), ((), ())),
                                preferred_element_type=jnp.float32)
            if slot == 0:
                s = s + bias[0]
            elif slot > WIN:
                s = s + bias[slot - WIN]
            top = jnp.max(s, axis=1, keepdims=True)
            if 0 < slot <= WIN:
                top = jnp.where(present[slot - 1], top, LOW)
            scores.append(s)
            tops.append(top)
        top = functools.reduce(jnp.maximum, tops) * SCALE
        total = None
        numerator = None
        for slot in range(SLOTS):
            shift = jnp.where(present[slot - 1], top, -LOW) if 0 < slot <= WIN else top
            w = jnp.exp2(scores[slot] * SCALE - shift)
            total = w if total is None else total + w
            term = jnp.dot(w.astype(jnp.bfloat16), kv[slot, head, 1],
                           preferred_element_type=jnp.float32)
            numerator = term if numerator is None else numerator + term
        total = jnp.sum(total, axis=1, keepdims=True)
        part(out_ref, head)[...] = (numerator / total).astype(out_ref.dtype)

    def first(head, carry):
        own(head)
        return carry

    lax.fori_loop(0, AHEAD, first, 0)
    q_copy.wait()

    def step(t, carry):
        @pl.when(t + AHEAD < heads)
        def _():
            own(t + AHEAD)

        for stage in range(1, STAGES):
            head = t - (stage - 1)

            @pl.when(both(head >= 0, head < heads))
            def _():
                relay(stage, head)

        head = t - (STAGES - 1)

        @pl.when(head >= 0)
        def _():
            leaves(head)
            attend(head)

        return carry

    lax.fori_loop(0, heads + STAGES - 1, step, 0)

    def sent(slot, parity, sem):
        size = heads if parity is None else (heads + 1 - parity) // 2
        ref = kv.at[slot, pl.ds(0, size)]
        pltpu.make_async_remote_copy(
            src_ref=ref, dst_ref=ref, send_sem=send_sem.at[sem], recv_sem=recv_sem.at[0, 0],
            device_id={"tm": block}, device_id_type=pl.DeviceIdType.MESH,
        ).wait_send()

    for mine in range(GROUP):

        @pl.when(role == mine)
        def _():
            for at, (_, slot, step_, dst, parity) in enumerate(sends_of(mine)):

                @pl.when(both(block >= slot, block + step_ < count))
                def _():
                    sent(slot, parity, at)

    @pl.when(tile + 1 < tiles)
    def _():
        sent(0, None, MOST)

    @pl.when(tile >= 1)
    def _():
        sent(0, None, MOST + 1)


def local(count, tiles, queries, keys, values, neighbours, halo_rows):
    frames, rows, columns, channels = queries.shape
    tokens = frames * rows * columns
    heads = channels // HD
    assert rows == HMAX and count % GROUP == 0
    flat = (tokens, channels)
    smem = pl.BlockSpec(memory_space=pltpu.SMEM)
    anywhere = pl.BlockSpec(memory_space=pl.ANY)
    out = pl.pallas_call(
        functools.partial(kernel, count, tiles, (frames, rows, columns)),
        out_shape=jax.ShapeDtypeStruct(flat, jnp.bfloat16),
        in_specs=[smem, smem, anywhere, anywhere, anywhere],
        out_specs=pl.BlockSpec(memory_space=pltpu.VMEM),
        scratch_shapes=[
            pltpu.VMEM((SLOTS, heads, 2, tokens, HD), jnp.bfloat16),
            pltpu.VMEM(flat, jnp.bfloat16),
            pltpu.VMEM((3, tokens, tokens), jnp.float32),
            pltpu.SemaphoreType.DMA((heads,)),
            pltpu.SemaphoreType.DMA,
            pltpu.SemaphoreType.DMA((MOST + 2,)),
            pltpu.SemaphoreType.DMA((SLOTS, heads)),
        ],
        compiler_params=pltpu.CompilerParams(
            collective_id=0, has_side_effects=True, vmem_limit_bytes=56 * 1024 * 1024
        ),
    )(
        neighbours.reshape(-1),
        halo_rows.reshape(-1),
        queries.reshape(flat),
        keys.reshape(flat),
        values.reshape(flat),
    )
    return out.reshape(queries.shape)


def solution(mesh):
    return jax.shard_map(
        functools.partial(local, mesh.shape["tm"], mesh.shape["tile"]),
        mesh=mesh,
        in_specs=(
            P("tm", "tile", None, None),
            P("tm", "tile", None, None),
            P("tm", "tile", None, None),
            P("tm", "tile", None),
            P("tm", "tile"),
        ),
        out_specs=P("tm", "tile", None, None),
        check_vma=False,
    )
```
